32 devices in a mesh: cfg: 2 (over x), seq: 16 (over z, y, core).
Axes of the slice: x: 2, y: 2, z: 4, core: 2. Of those that a mesh axis runs over, the one named last changes fastest.
Arguments:
- latent: bfloat16 [16, 1024, 1536], P('seq'), may hold values from -6 to 6
- text_ids: int32 [2, 512], P('cfg'), may hold values from 0 to 32127
- timestep: int32 [1], replicated, may hold values from 0 to 999
- guide_num: int32 [1], replicated, may hold values from 1024 to 8192
- guide_den: int32 [1], replicated, may hold values from 512 to 1024
- text_table: bfloat16 [32128, 1536], P('seq'), may hold values from -6 to 6
- time_in: bfloat16 [256, 1536], replicated, may hold values from -0.375 to 0.375
- time_out: bfloat16 [1536, 1536], P(None, 'seq'), may hold values from -0.15625 to 0.15625
- mod_weight: bfloat16 [1536, 7680], P(None, 'seq'), may hold values from -0.109375 to 0.109375
- qkv_weight: bfloat16 [1536, 4608], replicated, may hold values from -1 to 1
- out_weight: bfloat16 [1536, 1536], replicated, may hold values from -0.625 to 0.625
- head_weight: bfloat16 [1536, 64], replicated, may hold values from -0.15625 to 0.15625
Outputs:
- guided: float32 [16, 1024, 64], P('seq')
The draws below stay inside these ranges and needn't reach their ends.
All inputs are finite; a program needn't handle non-finite values.
Results may differ from the reference program's by a relative error of at most 0.0117.
Values may be sent and summed in bfloat16 or wider, within the bound.
A program may use at most 128 MiB of HBM per device.

```python
import math
import jax
import jax.numpy as jnp
import numpy as np
from jax import lax

D = 1536
HEADS = 24
OUT_CH = 64
VOCAB = 32128
FREQ = 256
TEXT = 512
PIXELS = 1024
FRAMES = 16
N_SEQ = 16


def draw_qkv_weight(key, part):
    base_key, head_key = jax.random.split(jax.random.fold_in(key, 17))
    spread_scale = 1.0 / math.sqrt(D)
    entries = jax.random.truncated_normal(base_key, -4.0, 4.0, (D, 3 * D), jnp.float32) * spread_scale
    return jnp.clip(entries, -1.0, 1.0).astype(jnp.bfloat16)


def touch_ends(result, stream_key, least, top_value):
    longest = result.shape.index(max(result.shape))
    spots = []
    for shift in (0, 1):
        where = [jax.random.randint(jax.random.fold_in(stream_key, axis), (), 0, length) for axis, length in enumerate(result.shape)]
        where[longest] = (where[longest] + shift) % result.shape[longest]
        spots.append(tuple(where))
    return result.at[spots[0]].set(least).at[spots[1]].set(top_value)


def block_levels(stream_key, dims, cuts, low, high):
    def one(dim, parts):
        heights = jax.random.uniform(jax.random.fold_in(jax.random.fold_in(stream_key, 6), dim), (parts,), jnp.float32, low / len(cuts), high / len(cuts))
        return jnp.repeat(jnp.exp(heights), dims[dim] // parts).reshape((-1,) + (1,) * (len(dims) - dim - 1))

    loudness = one(*cuts[0])
    for cut in cuts[1:]:
        loudness = loudness * one(*cut)
    return loudness


def rank_table(amount, skew):
    weights = [(1 << 20) // math.isqrt(rank ** skew) + 1 for rank in range(1, amount + 1)]
    width = 1 + sum(weights) // (1 << 30)
    return np.cumsum(np.array([max(1, weight // width) for weight in weights]))


def ranked(stream_key, dims, count, skew):
    table = rank_table(count, skew)
    pick = jax.random.randint(jax.random.fold_in(stream_key, 1), dims, 0, int(table[count - 1]))
    rank = jnp.searchsorted(jnp.asarray(table, jnp.int32), pick, side="right")
    return jax.random.permutation(jax.random.fold_in(stream_key, 2), count)[rank].astype(jnp.int32)


def scatter_about(rng, shape, scale, reach, shards=(), kind=jnp.bfloat16):
    drawn = jax.random.normal(rng, shape, jnp.float32) * scale
    if len(shards) > 0:
        drawn = block_levels(rng, shape, shards, -0.22, 0.18) * drawn
    return jnp.clip(drawn, min=-reach, max=reach).astype(kind)


def setup_inputs(seed: int = 0) -> dict:
    seeds = jax.random.split(jax.random.key(seed), 13)
    return {
        "latent": scatter_about(seeds[0], (FRAMES, PIXELS, D), 1.0, 6.0, ((0, 16),)),
        "text_ids": touch_ends(ranked(seeds[1], (2, TEXT), VOCAB, 1), jax.random.fold_in(seeds[1], 3), 0, VOCAB - 1).astype(jnp.int32),
        "timestep": jax.random.randint(seeds[2], (1,), 0, 1000).astype(jnp.int32),
        "guide_num": jax.random.randint(seeds[3], (1,), 1024, 8193).astype(jnp.int32),
        "guide_den": jax.random.randint(seeds[4], (1,), 512, 1025).astype(jnp.int32),
        "text_table": scatter_about(seeds[5], (VOCAB, D), 1.0, 6.0, ((0, 16),)),
        "time_in": scatter_about(seeds[6], (FREQ, D), FREQ ** -0.5, 0.375),
        "time_out": scatter_about(seeds[7], (D, D), D ** -0.5, 0.15625, ((1, 16),)),
        "mod_weight": scatter_about(seeds[8], (D, 5 * D), (2 * D) ** -0.5, 0.109375, ((1, 16),)),
        "qkv_weight": draw_qkv_weight(jax.random.fold_in(seeds[12], 71), 0),
        "out_weight": scatter_about(seeds[10], (D, D), (D // 16) ** -0.5, 0.625),
        "head_weight": scatter_about(seeds[11], (D, OUT_CH), D ** -0.5, 0.15625),
    }


norm_floor = 0.1

def layer_norm(values):
    center = values - lax.optimization_barrier(jnp.mean(values, axis=-1, keepdims=True))
    spread = lax.optimization_barrier(jnp.mean(center * center, axis=-1, keepdims=True))
    return center * lax.rsqrt(spread + norm_floor)

def modulate(values, shift_part, scale_part):
    return (layer_norm(values) * (1.0 + scale_part) + shift_part).astype(jnp.bfloat16)

def time_features(timestep):
    half_width = FREQ // 2
    ladder = jnp.arange(half_width, dtype=jnp.float32)
    freq_rates = jnp.exp(-math.log(10000.0) * ladder / half_width)
    angles = timestep.astype(jnp.float32)[0] * freq_rates
    return jnp.concatenate([jnp.cos(angles), jnp.sin(angles)])[None, :].astype(jnp.bfloat16)

def temporal_mix(normed, qkv_weight):
    frame_count, item_count, model_width = normed.shape
    head_dim = model_width // HEADS
    projected = jnp.dot(normed.reshape(-1, model_width), qkv_weight, preferred_element_type=jnp.float32)
    qkv_parts = []
    for part_index in range(3):
        rounded = projected[:, part_index * model_width:(part_index + 1) * model_width].astype(jnp.bfloat16)
        rounded = lax.optimization_barrier(rounded)
        qkv_parts.append(rounded.astype(jnp.float32).reshape(frame_count, item_count, HEADS, head_dim))
    scores = jnp.einsum('fphd,gphd->phfg', qkv_parts[0], qkv_parts[1]) * (1.0 / math.sqrt(head_dim))
    attn_prob = lax.optimization_barrier(jax.nn.softmax(scores, axis=-1).astype(jnp.bfloat16))
    mixed_rows = jnp.einsum('phfg,gphd->fphd', attn_prob.astype(jnp.float32), qkv_parts[2])
    return mixed_rows.astype(jnp.bfloat16).reshape(frame_count, item_count, model_width)

def finish_tokens(latent_part, mixed_rows, out_weight, head_weight, gate_attn, shift_out, scale_out):
    model_width = latent_part.shape[-1]
    base_rows = latent_part.reshape(-1, model_width).astype(jnp.float32)
    branch = jnp.dot(mixed_rows.reshape(-1, model_width), out_weight, preferred_element_type=jnp.float32)
    residual = base_rows + gate_attn * branch
    final_in = modulate(residual, shift_out, scale_out)
    prediction = jnp.dot(final_in, head_weight, preferred_element_type=jnp.float32)
    return prediction.reshape(latent_part.shape[:-1] + (head_weight.shape[1],))

def block_pass(latent_block, modulation, qkv_weight, out_weight, head_weight):
    shift_attn, scale_attn, gate_attn, shift_out, scale_out = jnp.split(modulation, 5)
    normed = modulate(latent_block.astype(jnp.float32), shift_attn, scale_attn)
    mixed_rows = temporal_mix(normed, qkv_weight)
    return finish_tokens(latent_block, mixed_rows, out_weight, head_weight, gate_attn, shift_out, scale_out)

def reference(latent, text_ids, timestep, guide_num, guide_den, text_table, time_in, time_out, mod_weight, qkv_weight, out_weight, head_weight):
    time_hidden = jax.nn.silu(jnp.dot(time_features(timestep), time_in, preferred_element_type=jnp.float32)).astype(jnp.bfloat16)
    time_embed = jnp.dot(time_hidden, time_out, preferred_element_type=jnp.float32)[0]
    blocks = PIXELS // N_SEQ
    by_block = jnp.transpose(latent.reshape(FRAMES, N_SEQ, blocks, D), (1, 0, 2, 3))
    predictions = []
    for pass_index in range(2):
        ids_row = text_ids[pass_index]
        pooled = lax.optimization_barrier(jnp.sum(jnp.take(text_table, ids_row, axis=0).astype(jnp.float32), axis=0)) / jnp.sqrt(jnp.float32(TEXT))
        cond_vec = jax.nn.silu(time_embed + pooled).astype(jnp.bfloat16)
        modulation = jnp.dot(cond_vec[None, :], mod_weight, preferred_element_type=jnp.float32)[0]

        def run_block(latent_block):
            return block_pass(latent_block, modulation, qkv_weight, out_weight, head_weight)
        prediction = lax.map(run_block, by_block)
        predictions.append(jnp.transpose(prediction, (1, 0, 2, 3)).reshape(FRAMES, PIXELS, OUT_CH))
    guide_scale = guide_num[0].astype(jnp.float32) / guide_den[0].astype(jnp.float32)
    return predictions[1] + guide_scale * (predictions[0] - predictions[1])
```

```python
import functools
import math

import jax
import jax.numpy as jnp
from jax import lax
from jax.experimental import pallas as pl
from jax.experimental.pallas import tpu as pltpu
from jax.sharding import PartitionSpec as P

HEADS = 24
FREQ = 256
NORM_FLOOR = 0.1
GROUP = 8
PACK = 2
BATCH = 2
FIRST_FAR = 2
SECOND_FAR = 6
VMEM_BYTES = 60 * 1024 * 1024
MESH = pl.DeviceIdType.MESH


def layer_norm(values):
    center = values - jnp.mean(values, axis=-1, keepdims=True)
    spread = jnp.mean(center * center, axis=-1, keepdims=True)
    return center * lax.rsqrt(spread + NORM_FLOOR)


def silu(values):
    return values / (1.0 + jnp.exp(-values))


def each(low, high, act):
    def run(k, carry):
        act(k)
        return carry

    lax.fori_loop(low, high, run, 0)


def whole_kernel(
    n_cfg, n_seq, head_dim, step_ref, num_ref, den_ref, ids_ref, latent_ref, table_hbm, tin_hbm,
    tout_hbm, mod_w_hbm, wqkv_hbm, wo_hbm, wh_hbm, out_ref,
    table, tin, tout, mod_w, wqkv, wo, wh, lat, slots, mods, mod_all, normed, qkv, mixed, preds,
    landed, load_sem, msg_send, msg_recv, near_send, near_recv, far_send, far_recv, mod_send,
    mod_recv, ret_send, ret_recv,
):
    cfg, me = lax.axis_index("cfg"), lax.axis_index("seq")
    total = n_cfg * n_seq
    mine = cfg * n_seq + me
    half_seq = n_seq // 2
    side, spot = me // half_seq, lax.rem(me, half_seq)
    frames, pixels, width = latent_ref.shape
    items = pixels // n_cfg // n_seq
    groups, all_frames = lat.shape[0], lat.shape[1]
    rows = all_frames * GROUP
    part_rows = rows // 2
    part_frames = all_frames // 2
    tokens = ids_ref.shape[1]
    voc = table.shape[0]
    out_ch = wh.shape[0] // PACK
    pairs = preds.shape[0]

    loads = []
    for n, (src, dst) in enumerate(
        (
            (table_hbm, table), (tin_hbm, tin), (tout_hbm, tout), (mod_w_hbm, mod_w),
            (wqkv_hbm, wqkv), (wo_hbm, wo), (wh_hbm, wh.at[:out_ch]), (wh_hbm, wh.at[out_ch:]),
        )
    ):
        loads.append(pltpu.make_async_copy(src, dst, load_sem.at[n]))
    for n in range(4):
        loads[n].start()

    def device(flat):
        return (flat // n_seq, lax.rem(flat, n_seq))

    barrier = pltpu.get_barrier_semaphore()
    each(1, total, lambda k: pl.semaphore_signal(
        barrier, inc=1, device_id=device(lax.rem(mine + k, total)), device_id_type=MESH
    ))

    def piece(owner, g):
        start = pl.multiple_of(cfg * (pixels // n_cfg) + owner * items + g * GROUP, GROUP)
        return latent_ref.at[:, pl.ds(start, GROUP), :]

    def place(source, at_side):
        return lax.rem(source + n_seq - at_side * half_seq, n_seq) * frames

    def near_copy(g, k):
        peer = side * half_seq + lax.rem(spot + k, half_seq)
        return pltpu.make_async_remote_copy(
            src_ref=piece(peer, g), dst_ref=lat.at[g, pl.ds(place(me, side), frames)],
            send_sem=near_send.at[g, k], recv_sem=near_recv.at[g, k],
            device_id=(cfg, peer), device_id_type=MESH,
        )

    def far_copy(g, k):
        peer = (1 - side) * half_seq + lax.rem(spot + k, half_seq)
        return pltpu.make_async_remote_copy(
            src_ref=piece(peer, g), dst_ref=lat.at[g, pl.ds(place(me, 1 - side), frames)],
            send_sem=far_send.at[g, k], recv_sem=far_recv.at[g, k],
            device_id=(cfg, peer), device_id_type=MESH,
        )

    def own_copy(g):
        return pltpu.make_async_copy(
            piece(me, g), lat.at[g, pl.ds(place(me, side), frames)], near_send.at[g, 0]
        )

    def msg_copy(k):
        peer = lax.rem(me + k, n_seq)
        return pltpu.make_async_remote_copy(
            src_ref=slots.at[me], dst_ref=slots.at[me], send_sem=msg_send.at[k],
            recv_sem=msg_recv.at[k], device_id=(cfg, peer), device_id_type=MESH,
        )

    def mod_copy(k):
        return pltpu.make_async_remote_copy(
            src_ref=mods.at[mine], dst_ref=mods.at[mine], send_sem=mod_send.at[k],
            recv_sem=mod_recv.at[k], device_id=device(lax.rem(mine + k, total)),
            device_id_type=MESH,
        )

    def ret_copy(q, k):
        flat = lax.rem(mine + k, total)
        return pltpu.make_async_remote_copy(
            src_ref=preds.at[q, pl.ds(place(lax.rem(flat, n_seq), side), frames)],
            dst_ref=landed.at[q, mine], send_sem=ret_send.at[q, k], recv_sem=ret_recv.at[q, k],
            device_id=device(flat), device_id_type=MESH,
        )

    ids = jnp.broadcast_to(ids_ref[...] - me * voc, (128, tokens)).T
    lanes = lax.broadcasted_iota(jnp.int32, (tokens, 128), 1)
    tiles = []
    for t in range(-(-voc // 128)):
        hits = jnp.where(ids == lanes + t * 128, 1.0, 0.0)
        tiles.append(jnp.sum(hits, axis=0, keepdims=True))
    counts = jnp.concatenate(tiles, axis=1)[:, :voc]
    high = jnp.floor(counts * (1.0 / 256.0)) * 256.0
    counts = jnp.concatenate([high, counts - high], axis=0).astype(jnp.bfloat16)

    pl.semaphore_wait(barrier, total - 1)
    each(0, FIRST_FAR, lambda k: far_copy(0, k).start())
    own_copy(0).start()
    each(1, half_seq, lambda k: near_copy(0, k).start())

    time = jnp.full((1, FREQ // 2), step_ref[0], jnp.int32).astype(jnp.float32)
    ladder = lax.broadcasted_iota(jnp.int32, (1, FREQ // 2), 1).astype(jnp.float32)
    angles = time * jnp.exp(-math.log(10000.0) * ladder / (FREQ // 2))
    time_freq = jnp.concatenate([jnp.cos(angles), jnp.sin(angles)], axis=1).astype(jnp.bfloat16)
    loads[1].wait()
    hidden = silu(jnp.dot(time_freq, tin[...], preferred_element_type=jnp.float32))
    loads[2].wait()
    time_part = lax.dot_general(
        hidden.astype(jnp.bfloat16), tout[...], (((1,), (1,)), ((), ())),
        preferred_element_type=jnp.float32,
    )
    lane = lax.broadcasted_iota(jnp.int32, (1, width), 1)
    first = me * tout.shape[0]
    placed = jnp.where(
        (lane >= first) & (lane < first + tout.shape[0]),
        jnp.concatenate([time_part] * n_seq, axis=1), 0.0,
    )

    loads[0].wait()
    for n in range(4, 8):
        loads[n].start()
    sums = jnp.dot(counts, table[...], preferred_element_type=jnp.float32)
    pooled = jnp.sum(sums, axis=0, keepdims=True) * (1.0 / math.sqrt(tokens))
    slots[me] = pooled + placed
    each(1, n_seq, lambda k: msg_copy(k).start())
    each(FIRST_FAR, SECOND_FAR, lambda k: far_copy(0, k).start())
    for g in range(1, min(2, groups)):
        own_copy(g).start()
        each(1, half_seq, lambda k: near_copy(g, k).start())
    loads[3].wait()
    each(1, n_seq, lambda k: msg_copy(k).wait())
    cond = silu(jnp.sum(slots[...], axis=0)).astype(jnp.bfloat16)
    mods[mine] = lax.dot_general(
        cond, mod_w[...], (((1,), (1,)), ((), ())), preferred_element_type=jnp.float32
    )
    each(1, total, lambda k: mod_copy(k).start())
    each(SECOND_FAR, half_seq, lambda k: far_copy(0, k).start())
    for g in range(2, groups):
        own_copy(g).start()
        each(1, half_seq, lambda k: near_copy(g, k).start())
    for g in range(1, groups):
        each(0, half_seq, lambda k: far_copy(g, k).start())
    each(1, total, lambda k: mod_copy(k).wait())
    for c in range(n_cfg):
        mod_all[c : c + 1] = jnp.concatenate(
            [mods[c * n_seq + s] for s in range(n_seq)], axis=1
        )
    for n in range(4, 8):
        loads[n].wait()

    def modulation(c, n):
        return mod_all[c : c + 1, n * width : (n + 1) * width]

    def modulated(g, where, at):
        x = lat[g, where].astype(jnp.float32).reshape(part_rows, width)
        n = layer_norm(x)
        for c in range(n_cfg):
            y = n * (1.0 + modulation(c, 1)) + modulation(c, 0)
            start = at + c * part_rows
            normed[start : start + part_rows, :] = y.astype(jnp.bfloat16)

    chunk = 4 * head_dim
    steps = width // chunk

    def project(x, j, part):
        at = slice(part * width + j * chunk, part * width + (j + 1) * chunk)
        out = jnp.dot(x, wqkv[:, at], preferred_element_type=jnp.float32)
        if part == 0:
            out = out * (1.0 / math.sqrt(head_dim))
        return at, out.astype(jnp.bfloat16)

    batch = min(BATCH, groups)

    def near_wave(b, carry):
        for n in range(batch):
            g = b * batch + n
            own_copy(g).wait()
            each(1, half_seq, lambda k: near_copy(g, k).wait_recv())
        for n in range(batch):
            modulated(b * batch + n, slice(0, part_frames), n * n_cfg * part_rows)
        x = normed[...]
        for j in range(steps):
            for part in range(3):
                at, out = project(x, j, part)
                for n in range(batch):
                    for c in range(n_cfg):
                        start = (n * n_cfg + c) * part_rows
                        qkv[b * batch + n, c, :part_rows, at] = out[start : start + part_rows]
        return carry

    lax.fori_loop(0, groups // batch, near_wave, 0)

    pair = 2 * head_dim
    lane = lax.broadcasted_iota(jnp.int32, (1, pair), 1)
    left = jnp.where(lane < head_dim, 1.0, 0.0).astype(jnp.bfloat16)
    right = jnp.where(lane < head_dim, 0.0, 1.0).astype(jnp.bfloat16)
    same = lax.broadcasted_iota(jnp.int32, (1, GROUP, rows), 1) == lax.rem(
        lax.broadcasted_iota(jnp.int32, (1, GROUP, rows), 2), GROUP
    )
    shares = jnp.concatenate(
        [jnp.broadcast_to(left, (rows, pair)), jnp.broadcast_to(right, (rows, pair))], axis=0
    )
    top = jnp.full((1, PACK * out_ch), num_ref[0], jnp.int32).astype(jnp.float32)
    bottom = jnp.full((1, PACK * out_ch), den_ref[0], jnp.int32).astype(jnp.float32)
    guide_scale = top / bottom

    def attend(g, c, start):
        q = qkv[g, c, :, start : start + pair]
        kk = qkv[g, c, :, width + start : width + start + pair]
        vv = qkv[g, c, :, 2 * width + start : 2 * width + start + pair]
        keys = jnp.concatenate([kk * left, kk * right], axis=0)
        vals = jnp.concatenate([vv * left, vv * right], axis=0)
        vals = jnp.concatenate([vals, shares], axis=1)
        scores = lax.dot_general(
            q, keys, (((1,), (1,)), ((), ())), preferred_element_type=jnp.float32
        )
        probs = []
        for s in range(2):
            t = scores[:, s * rows : (s + 1) * rows].reshape(all_frames, GROUP, rows)
            t = jnp.where(same, t, -jnp.inf).reshape(rows, rows)
            e = jnp.exp(t - jnp.max(t, axis=1, keepdims=True))
            probs.append(e.astype(jnp.bfloat16))
        both = jnp.dot(
            jnp.concatenate(probs, axis=1), vals, preferred_element_type=jnp.float32
        )
        o = both[:, :pair] / both[:, pair:]
        mixed[c * rows : (c + 1) * rows, start : start + pair] = o.astype(jnp.bfloat16)

    def far_wave(g, carry):
        each(0, half_seq, lambda k: far_copy(g, k).wait_recv())
        modulated(g, slice(part_frames, all_frames), 0)
        x = normed[: n_cfg * part_rows]

        def extend(j):
            for part in range(3):
                at, out = project(x, j, part)
                for c in range(n_cfg):
                    qkv[g, c, part_rows:, at] = out[c * part_rows : (c + 1) * part_rows]

        extend(0)
        for j in range(steps):
            if j + 1 < steps:
                extend(j + 1)
            for c in range(n_cfg):
                for h in range(chunk // pair):
                    attend(g, c, j * chunk + h * pair)
        branch = jnp.dot(mixed[...], wo[...], preferred_element_type=jnp.float32)
        x = lat[g].astype(jnp.float32).reshape(rows, width)
        finals = []
        for c in range(n_cfg):
            residual = x + modulation(c, 2) * branch[c * rows : (c + 1) * rows]
            final = layer_norm(residual) * (1.0 + modulation(c, 4)) + modulation(c, 3)
            finals.append(final.astype(jnp.bfloat16))
        both = lax.dot_general(
            jnp.concatenate(finals, axis=0), wh[...], (((1,), (1,)), ((), ())),
            preferred_element_type=jnp.float32,
        )
        guided = both[rows:] + guide_scale * (both[:rows] - both[rows:])
        guided = guided.reshape(all_frames, GROUP, PACK * out_ch).astype(preds.dtype)
        q = g // PACK

        @pl.when(lax.rem(g, PACK) == 0)
        def _():
            preds[q] = guided

        @pl.when(lax.rem(g, PACK) != 0)
        def _():
            preds[q, :, :, out_ch:] = guided[:, :, out_ch:]

        @pl.when((lax.rem(g, PACK) == PACK - 1) | (g == groups - 1))
        def _():
            each(1, total, lambda k: ret_copy(q, k).start())
            landed[q, mine] = preds[q, pl.ds(place(me, side), frames)]

        return carry

    lax.fori_loop(0, groups, far_wave, 0)

    for g in range(groups):
        each(1, half_seq, lambda k: near_copy(g, k).wait_send())
        each(0, half_seq, lambda k: far_copy(g, k).wait_send())
    for q in range(pairs):
        each(1, total, lambda k: ret_copy(q, k).wait())
    for f in range(frames):
        slabs = []
        for source in range(total):
            for g in range(groups):
                slab = landed[g // PACK, source, f].astype(jnp.float32)
                if g % PACK:
                    slab = pltpu.roll(slab, out_ch, 1)
                slabs.append(slab)
        per = 128 // GROUP
        for n in range(pixels // 128):
            block = jnp.concatenate(slabs[n * per : (n + 1) * per], axis=0)
            out_ref[f, :, n * 128 : (n + 1) * 128] = block.T[:out_ch]


def whole(step, num, den, ids, latent, table, tin, tout, mod_w, wqkv, wo, wh):
    n_cfg, n_seq = lax.axis_size("cfg"), lax.axis_size("seq")
    frames, pixels, width = latent.shape
    head_dim = width // HEADS
    items = pixels // n_cfg // n_seq
    groups, all_frames = items // GROUP, frames * n_seq
    rows = all_frames * GROUP
    total = n_cfg * n_seq
    half_seq = n_seq // 2
    batch = min(BATCH, groups)
    pairs = -(-groups // PACK)
    mod_cols = mod_w.shape[0]
    out_ch = wh.shape[0]
    smem = pl.BlockSpec(memory_space=pltpu.SMEM)
    vmem = pl.BlockSpec(memory_space=pltpu.VMEM)
    hbm = pl.BlockSpec(memory_space=pl.ANY)
    bf16 = jnp.bfloat16
    dma = pltpu.SemaphoreType.DMA
    return pl.pallas_call(
        functools.partial(whole_kernel, n_cfg, n_seq, head_dim),
        out_shape=jax.ShapeDtypeStruct((frames, out_ch, pixels), jnp.float32),
        in_specs=[smem, smem, smem, vmem, hbm, hbm, hbm, hbm, hbm, hbm, hbm, hbm],
        out_specs=vmem,
        scratch_shapes=[
            pltpu.VMEM(table.shape, bf16),
            pltpu.VMEM(tin.shape, bf16),
            pltpu.VMEM(tout.shape, bf16),
            pltpu.VMEM(mod_w.shape, bf16),
            pltpu.VMEM(wqkv.shape, bf16),
            pltpu.VMEM(wo.shape, bf16),
            pltpu.VMEM((PACK * out_ch, width), bf16),
            pltpu.VMEM((groups, all_frames, GROUP, width), bf16),
            pltpu.VMEM((n_seq, 1, width), jnp.float32),
            pltpu.VMEM((total, 1, mod_cols), jnp.float32),
            pltpu.VMEM((n_cfg, n_seq * mod_cols), jnp.float32),
            pltpu.VMEM((batch * n_cfg * rows // 2, width), bf16),
            pltpu.VMEM((groups, n_cfg, rows, 3 * width), bf16),
            pltpu.VMEM((n_cfg * rows, width), bf16),
            pltpu.VMEM((pairs, all_frames, GROUP, PACK * out_ch), bf16),
            pltpu.VMEM((pairs, total, frames, GROUP, PACK * out_ch), bf16),
            dma((8,)),
            dma((n_seq,)), dma((n_seq,)),
            dma((groups, half_seq)), dma((groups, half_seq)),
            dma((groups, half_seq)), dma((groups, half_seq)),
            dma((total,)), dma((total,)),
            dma((pairs, total)), dma((pairs, total)),
        ],
        compiler_params=pltpu.CompilerParams(
            collective_id=0, has_side_effects=True, vmem_limit_bytes=VMEM_BYTES
        ),
        name="whole",
    )(step, num, den, ids, latent, table, tin, tout, mod_w, wqkv, wo, wh)


def on_device(
    latent, text_ids, timestep, guide_num, guide_den, text_table,
    time_in, time_out, mod_weight, qkv_weight, out_weight, head_weight,
):
    out = whole(
        timestep, guide_num, guide_den, text_ids, latent, text_table, time_in, time_out.T,
        mod_weight.T, qkv_weight, out_weight, head_weight.T,
    )
    return jnp.swapaxes(out, 1, 2)


def solution(mesh):
    in_specs = (
        P("seq", None, None), P("cfg", None), P(), P(), P(), P("seq", None),
        P(), P(None, "seq"), P(None, "seq"), P(), P(), P(),
    )
    return jax.shard_map(
        on_device, mesh=mesh, in_specs=in_specs, out_specs=P("seq", None, None), check_vma=False
    )
```

```python
import functools
import math

import jax
import jax.numpy as jnp
from jax import lax
from jax.experimental import pallas as pl
from jax.experimental.pallas import tpu as pltpu
from jax.sharding import PartitionSpec as P

HEADS = 24
FREQ = 256
NORM_FLOOR = 0.1
GROUP = 8
PACK = 2
EDGE_EARLY = 5
MIDDLE_EARLY = 8
AHEAD = 2
NEAR_EARLY = 2
SLICE = 512
VMEM_BYTES = 60 * 1024 * 1024
MESH = pl.DeviceIdType.MESH


def layer_norm(values):
    center = values - jnp.mean(values, axis=-1, keepdims=True)
    spread = jnp.mean(center * center, axis=-1, keepdims=True)
    return center * lax.rsqrt(spread + NORM_FLOOR)


def silu(values):
    return values / (1.0 + jnp.exp(-values))


def each(low, high, act):
    def run(k, carry):
        act(k)
        return carry

    lax.fori_loop(low, high, run, 0)


def whole_kernel(
    n_cfg, n_seq, head_dim, step_hbm, num_hbm, den_hbm, ids_hbm, latent_ref, table_hbm, tin_hbm,
    tout_hbm, mod_w_hbm, wqkv_hbm, wo_hbm, wh_hbm, out_ref,
    step, num, den, ids_ref, table, tin, tout, mod_w, wqkv, wo, wh, lat, slots, mods, mod_all,
    normed, qkv, mixed, branch, finals, spare, preds, landed, load_sem, msg_sem, mod_sem, own_sem,
    lat_sem, ret_send, ret_recv,
):
    cfg, me = lax.axis_index("cfg"), lax.axis_index("seq")
    total = n_cfg * n_seq
    mine = cfg * n_seq + me
    half_seq = n_seq // 2
    side, spot = me // half_seq, lax.rem(me, half_seq)
    edge = jnp.where((2 * me // half_seq == 0) | (2 * me // half_seq == 3), 1, 0)
    early = min(MIDDLE_EARLY, half_seq) + edge * (min(EDGE_EARLY, half_seq) - min(MIDDLE_EARLY, half_seq))
    frames, pixels, width = latent_ref.shape
    items = pixels // n_cfg // n_seq
    groups, all_frames = lat.shape[0], lat.shape[1]
    rows = all_frames * GROUP
    part_rows, part_frames = rows // 2, all_frames // 2
    tokens = ids_ref.shape[1]
    voc = table.shape[0]
    out_ch = wh.shape[0] // PACK
    pairs = preds.shape[0]
    batch = normed.shape[0] // rows * 2 // n_cfg

    loads = []
    for n, (src, dst) in enumerate(
        (
            (ids_hbm, ids_ref), (step_hbm, step), (tin_hbm, tin), (tout_hbm, tout),
            (mod_w_hbm, mod_w), (num_hbm, num), (den_hbm, den),
            (wqkv_hbm, wqkv), (wo_hbm, wo), (wh_hbm, wh.at[:out_ch]), (wh_hbm, wh.at[out_ch:]),
        )
    ):
        loads.append(pltpu.make_async_copy(src, dst, load_sem.at[n]))
    cuts = list(range(0, voc, SLICE)) + [voc]
    strips = []
    for n, (low, high) in enumerate(zip(cuts[:-1], cuts[1:])):
        strip = slice(low, high)
        strips.append((strip, pltpu.make_async_copy(
            table_hbm.at[strip], table.at[strip], load_sem.at[len(loads) + n]
        )))
    loads[0].start()
    loads[1].start()
    loads[2].start()
    strips[0][1].start()
    loads[3].start()
    for _, strip_copy in strips[1:]:
        strip_copy.start()

    def device(flat):
        return (flat // n_seq, lax.rem(flat, n_seq))

    barrier = pltpu.get_barrier_semaphore()
    each(1, total, lambda k: pl.semaphore_signal(
        barrier, inc=1, device_id=device(lax.rem(mine + k, total)), device_id_type=MESH
    ))

    def piece(owner, g):
        start = pl.multiple_of(cfg * (pixels // n_cfg) + owner * items + g * GROUP, GROUP)
        return latent_ref.at[:, pl.ds(start, GROUP), :]

    def place(source, at_side):
        return lax.rem(source + n_seq - at_side * half_seq, n_seq) * frames

    def near_copy(g, k):
        peer = side * half_seq + lax.rem(spot + k, half_seq)
        return pltpu.make_async_remote_copy(
            src_ref=piece(peer, g), dst_ref=lat.at[g, pl.ds(place(me, side), frames)],
            send_sem=lat_sem.at[2 * groups], recv_sem=lat_sem.at[g],
            device_id=(cfg, peer), device_id_type=MESH,
        )

    def far_copy(g, k):
        peer = (1 - side) * half_seq + lax.rem(spot + k, half_seq)
        return pltpu.make_async_remote_copy(
            src_ref=piece(peer, g), dst_ref=lat.at[g, pl.ds(place(me, 1 - side), frames)],
            send_sem=lat_sem.at[2 * groups], recv_sem=lat_sem.at[groups + g],
            device_id=(cfg, peer), device_id_type=MESH,
        )

    def own_copy(g):
        return pltpu.make_async_copy(
            piece(me, g), lat.at[g, pl.ds(place(me, side), frames)], own_sem.at[g]
        )

    def send_near(g):
        own_copy(g).start()
        each(1, half_seq, lambda k: near_copy(g, k).start())

    def send_far(g, low, high):
        each(low, high, lambda k: far_copy(g, k).start())

    def msg_copy(k):
        peer = lax.rem(me + k, n_seq)
        return pltpu.make_async_remote_copy(
            src_ref=slots.at[me], dst_ref=slots.at[me], send_sem=msg_sem.at[0],
            recv_sem=msg_sem.at[1], device_id=(cfg, peer), device_id_type=MESH,
        )

    def mod_copy(k):
        return pltpu.make_async_remote_copy(
            src_ref=mods.at[mine], dst_ref=mods.at[mine], send_sem=mod_sem.at[0],
            recv_sem=mod_sem.at[1], device_id=device(lax.rem(mine + k, total)),
            device_id_type=MESH,
        )

    def ret_copy(q, k):
        flat = lax.rem(mine + k, total)
        return pltpu.make_async_remote_copy(
            src_ref=preds.at[q, pl.ds(place(lax.rem(flat, n_seq), side), frames)],
            dst_ref=landed.at[q, mine], send_sem=ret_send.at[q], recv_sem=ret_recv.at[q],
            device_id=device(flat), device_id_type=MESH,
        )

    def drain(ref, sem):
        pltpu.make_async_copy(ref, ref, sem).wait()
    loads[0].wait()
    ids = jnp.broadcast_to(ids_ref[...] - me * voc, (128, tokens)).T
    lanes = lax.broadcasted_iota(jnp.int32, (tokens, 128), 1)
    tiles = []
    for t in range(-(-voc // 128)):
        hits = jnp.where(ids == lanes + t * 128, 1.0, 0.0)
        tiles.append(jnp.sum(hits, axis=0, keepdims=True))
    counts = jnp.concatenate(tiles, axis=1)[:, :voc]
    high = jnp.floor(counts * (1.0 / 256.0)) * 256.0
    counts = jnp.concatenate([high, counts - high], axis=0).astype(jnp.bfloat16)
    loads[1].wait()
    time = jnp.full((1, FREQ // 2), step[0], jnp.int32).astype(jnp.float32)
    ladder = lax.broadcasted_iota(jnp.int32, (1, FREQ // 2), 1).astype(jnp.float32)
    angles = time * jnp.exp(-math.log(10000.0) * ladder / (FREQ // 2))
    time_freq = jnp.concatenate([jnp.cos(angles), jnp.sin(angles)], axis=1).astype(jnp.bfloat16)
    loads[2].wait()
    hidden = silu(jnp.dot(time_freq, tin[...], preferred_element_type=jnp.float32))
    loads[3].wait()
    time_part = lax.dot_general(
        hidden.astype(jnp.bfloat16), tout[...], (((1,), (1,)), ((), ())),
        preferred_element_type=jnp.float32,
    )
    lane = lax.broadcasted_iota(jnp.int32, (1, width), 1)
    first = me * tout.shape[0]
    placed = jnp.where(
        (lane >= first) & (lane < first + tout.shape[0]),
        jnp.concatenate([time_part] * n_seq, axis=1), 0.0,
    )
    sums = jnp.zeros((2, width), jnp.float32)
    for strip, strip_copy in strips:
        strip_copy.wait()
        sums += jnp.dot(counts[:, strip], table[strip, :], preferred_element_type=jnp.float32)
    for n in range(4, 11):
        loads[n].start()
    pooled = jnp.sum(sums, axis=0, keepdims=True) * (1.0 / math.sqrt(tokens)) + placed
    wide = width // 2
    slots[me] = jnp.concatenate([pooled[:, :wide], pooled[:, wide:]], axis=0).astype(slots.dtype)
    pl.semaphore_wait(barrier, total - 1)
    each(1, n_seq, lambda k: msg_copy(k).start())
    for g in range(min(NEAR_EARLY, groups)):
        send_near(g)
    send_far(0, 0, early)
    loads[4].wait()
    drain(slots.at[pl.ds(0, n_seq - 1)], msg_sem.at[1])
    cond = silu(jnp.sum(slots[...].astype(jnp.float32), axis=0)).astype(jnp.bfloat16)
    cond = jnp.concatenate([cond[:1], cond[1:]], axis=1)
    mods[mine] = lax.dot_general(
        cond, mod_w[...], (((1,), (1,)), ((), ())), preferred_element_type=jnp.float32
    )
    each(1, total, lambda k: mod_copy(k).start())
    for g in range(min(NEAR_EARLY, groups), groups):
        send_near(g)
    send_far(0, early, half_seq)
    for g in range(1, groups):
        send_far(g, 0, half_seq if g < AHEAD else half_seq * edge)
    for n in range(5, 11):
        loads[n].wait()
    drain(mods.at[pl.ds(0, total - 1)], mod_sem.at[1])
    for c in range(n_cfg):
        mod_all[c : c + 1] = jnp.concatenate(
            [mods[c * n_seq + s] for s in range(n_seq)], axis=1
        )

    def modulation(c, n):
        return mod_all[c : c + 1, n * width : (n + 1) * width]

    chunk = 4 * head_dim
    steps = width // chunk
    pair = 2 * head_dim
    slab = rows // 4
    slab_frames = all_frames // 4
    lane = lax.broadcasted_iota(jnp.int32, (1, pair), 1)
    left = jnp.where(lane < head_dim, 1.0, 0.0).astype(jnp.bfloat16)
    right = jnp.where(lane < head_dim, 0.0, 1.0).astype(jnp.bfloat16)
    same = lax.broadcasted_iota(jnp.int32, (1, GROUP, rows), 1) == lax.rem(
        lax.broadcasted_iota(jnp.int32, (1, GROUP, rows), 2), GROUP
    )
    shares = jnp.concatenate(
        [jnp.broadcast_to(left, (rows, pair)), jnp.broadcast_to(right, (rows, pair))], axis=0
    )
    top = jnp.full((1, PACK * out_ch), num[0], jnp.int32).astype(jnp.float32)
    bottom = jnp.full((1, PACK * out_ch), den[0], jnp.int32).astype(jnp.float32)
    guide_scale = top / bottom

    def near_arrive(g):
        own_copy(g).wait()
        drain(lat.at[g, pl.ds(0, part_frames - frames)], lat_sem.at[g])

    def far_arrive(g):
        drain(lat.at[g, pl.ds(0, part_frames)], lat_sem.at[groups + g])

    def latent(g, r):
        x = lat[g, r * slab_frames : (r + 1) * slab_frames].astype(jnp.float32)
        return x.reshape(slab, width)

    def prepare(g, r, at):
        n = layer_norm(latent(g, r))
        for c in range(n_cfg):
            y = n * (1.0 + modulation(c, 1)) + modulation(c, 0)
            start = at + c * part_rows + (r % 2) * slab
            normed[start : start + slab, :] = y.astype(jnp.bfloat16)

    def project(owners, first, j):
        x = normed[: len(owners) * n_cfg * part_rows]
        for part in range(3):
            at = slice(part * width + j * chunk, part * width + (j + 1) * chunk)
            out = jnp.dot(x, wqkv[:, at], preferred_element_type=jnp.float32)
            if part == 0:
                out = out * (1.0 / math.sqrt(head_dim))
            out = out.astype(jnp.bfloat16)
            for n, g in enumerate(owners):
                for c in range(n_cfg):
                    start = (n * n_cfg + c) * part_rows
                    qkv[g, c, first : first + part_rows, at] = out[start : start + part_rows]

    def attend(g, c, h):
        at = slice(c * rows, (c + 1) * rows)
        kk = qkv[g, c, :, width + h * pair : width + (h + 1) * pair]
        vv = qkv[g, c, :, 2 * width + h * pair : 2 * width + (h + 1) * pair]
        keys = jnp.concatenate([kk * left, kk * right], axis=0)
        vals = jnp.concatenate([vv * left, vv * right], axis=0)
        vals = jnp.concatenate([vals, shares], axis=1)
        scores = lax.dot_general(
            qkv[g, c, :, h * pair : (h + 1) * pair], keys, (((1,), (1,)), ((), ())),
            preferred_element_type=jnp.float32,
        )
        probs = []
        for s in range(2):
            t = scores[:, s * rows : (s + 1) * rows].reshape(all_frames, GROUP, rows)
            t = jnp.where(same, t, -jnp.inf).reshape(rows, rows)
            e = jnp.exp(t - jnp.max(t, axis=1, keepdims=True))
            probs.append(e.astype(jnp.bfloat16))
        both = jnp.dot(
            jnp.concatenate(probs, axis=1), vals, preferred_element_type=jnp.float32
        )
        o = both[:, :pair] / both[:, pair:]
        mixed[at, h * pair : (h + 1) * pair] = o.astype(jnp.bfloat16)

    def leave(j):
        at = slice(j * chunk, (j + 1) * chunk)
        branch[:, at] = jnp.dot(mixed[...], wo[:, at], preferred_element_type=jnp.float32)

    def settle(g, r):
        x = latent(g, r)
        for c in range(n_cfg):
            start = c * rows + r * slab
            residual = x + modulation(c, 2) * branch[start : start + slab, :]
            final = layer_norm(residual) * (1.0 + modulation(c, 4)) + modulation(c, 3)
            finals[start : start + slab, :] = final.astype(jnp.bfloat16)

    def guide():
        both = lax.dot_general(
            finals[...], wh[...], (((1,), (1,)), ((), ())), preferred_element_type=jnp.float32
        )
        guided = both[rows:] + guide_scale * (both[:rows] - both[rows:])
        spare[...] = guided.reshape(all_frames, GROUP, PACK * out_ch).astype(spare.dtype)

    def give(g):
        q = g // PACK

        @pl.when(lax.rem(g, PACK) == 0)
        def _():
            preds[q] = spare[...]

        @pl.when(lax.rem(g, PACK) != 0)
        def _():
            preds[q, :, :, out_ch:] = spare[:, :, out_ch:]

        @pl.when((lax.rem(g, PACK) == PACK - 1) | (g == groups - 1))
        def _():
            each(1, total, lambda k: ret_copy(q, k).start())
            landed[q, mine] = preds[q, pl.ds(place(me, side), frames)]

    def attention(g):
        def one(n, carry):
            for c in range(n_cfg):
                for h in range(width // pair):
                    attend(g, c, h)
            return carry

        lax.fori_loop(0, 1, one, 0)

    def near_wave(b, carry):
        owners = [b * batch + n for n in range(batch)]
        for g in owners:
            near_arrive(g)
        for n, g in enumerate(owners):
            for r in range(2):
                prepare(g, r, n * n_cfg * part_rows)
        for j in range(steps):
            project(owners, 0, j)

        @pl.when(AHEAD + b < groups)
        def _():
            send_far(AHEAD + b, 0, half_seq * (1 - edge))
        return carry
    lax.fori_loop(0, groups // batch, near_wave, 0)
    for g in range(AHEAD + groups // batch, groups):
        send_far(g, 0, half_seq * (1 - edge))

    def far_wave(g, late):
        far_arrive(g)
        for r in range(2, 4):
            prepare(g, r, 0)
        for j in range(steps):
            project([g], part_rows, j)
            if j < len(late):
                late[j]()
        attention(g)

    def leave_all():
        for j in range(steps):
            leave(j)

    far_wave(jnp.int32(0), [])
    leave_all()

    def wave(g, carry):
        far_wave(g, [functools.partial(settle, g - 1, r) for r in range(4)] + [guide])
        give(g - 1)
        leave_all()
        return carry

    lax.fori_loop(1, groups, wave, 0)
    for r in range(4):
        settle(groups - 1, r)
    guide()
    give(jnp.int32(groups - 1))
    drain(slots.at[pl.ds(0, n_seq - 1)], msg_sem.at[0])
    drain(mods.at[pl.ds(0, total - 1)], mod_sem.at[0])
    drain(lat.at[:, pl.ds(0, all_frames - frames)], lat_sem.at[2 * groups])
    for q in range(pairs):
        drain(landed.at[q, pl.ds(0, total - 1)], ret_recv.at[q])
        drain(landed.at[q, pl.ds(0, total - 1)], ret_send.at[q])
    per = 128 // GROUP
    for f in range(frames):
        slabs = []
        for source in range(total):
            for g in range(groups):
                tile = landed[g // PACK, source, f].astype(jnp.float32)
                if g % PACK:
                    tile = pltpu.roll(tile, out_ch, 1)
                slabs.append(tile)
        for n in range(pixels // 128):
            block = jnp.concatenate(slabs[n * per : (n + 1) * per], axis=0)
            out_ref[f, :, n * 128 : (n + 1) * 128] = block.T[:out_ch]


def whole(step, num, den, ids, latent, table, tin, tout, mod_w, wqkv, wo, wh):
    n_cfg, n_seq = lax.axis_size("cfg"), lax.axis_size("seq")
    frames, pixels, width = latent.shape
    head_dim = width // HEADS
    items = pixels // n_cfg // n_seq
    groups, all_frames = items // GROUP, frames * n_seq
    rows = all_frames * GROUP
    total = n_cfg * n_seq
    pairs = -(-groups // PACK)
    mod_cols = mod_w.shape[0]
    out_ch = wh.shape[0]
    hbm = pl.BlockSpec(memory_space=pl.ANY)
    bf16 = jnp.bfloat16
    dma = pltpu.SemaphoreType.DMA
    return pl.pallas_call(
        functools.partial(whole_kernel, n_cfg, n_seq, head_dim),
        out_shape=pltpu.VMEM((frames, out_ch, pixels), jnp.float32),
        in_specs=[pl.BlockSpec(memory_space=pltpu.HBM)] * 3 + [hbm] * 9,
        out_specs=pl.BlockSpec(memory_space=pltpu.VMEM),
        scratch_shapes=[
            pltpu.SMEM((1,), jnp.int32),
            pltpu.SMEM((1,), jnp.int32),
            pltpu.SMEM((1,), jnp.int32),
            pltpu.VMEM(ids.shape, jnp.int32),
            pltpu.VMEM(table.shape, bf16),
            pltpu.VMEM(tin.shape, bf16),
            pltpu.VMEM(tout.shape, bf16),
            pltpu.VMEM(mod_w.shape, bf16),
            pltpu.VMEM(wqkv.shape, bf16),
            pltpu.VMEM(wo.shape, bf16),
            pltpu.VMEM((PACK * out_ch, width), bf16),
            pltpu.VMEM((groups, all_frames, GROUP, width), bf16),
            pltpu.VMEM((n_seq, 2, width // 2), bf16),
            pltpu.VMEM((total, 1, mod_cols), jnp.float32),
            pltpu.VMEM((n_cfg, n_seq * mod_cols), jnp.float32),
            pltpu.VMEM((min(2, groups) * n_cfg * rows // 2, width), bf16),
            pltpu.VMEM((groups, n_cfg, rows, 3 * width), bf16),
            pltpu.VMEM((n_cfg * rows, width), bf16),
            pltpu.VMEM((n_cfg * rows, width), jnp.float32),
            pltpu.VMEM((n_cfg * rows, width), bf16),
            pltpu.VMEM((all_frames, GROUP, PACK * out_ch), bf16),
            pltpu.VMEM((pairs, all_frames, GROUP, PACK * out_ch), bf16),
            pltpu.VMEM((pairs, total, frames, GROUP, PACK * out_ch), bf16),
            dma((11 + -(-table.shape[0] // SLICE),)), dma((2,)), dma((2,)), dma((groups,)),
            dma((2 * groups + 1,)), dma((pairs,)), dma((pairs,)),
        ],
        compiler_params=pltpu.CompilerParams(
            collective_id=0, has_side_effects=True, vmem_limit_bytes=VMEM_BYTES
        ),
        name="whole",
    )(step, num, den, ids, latent, table, tin, tout, mod_w, wqkv, wo, wh)


def on_device(
    latent, text_ids, timestep, guide_num, guide_den, text_table,
    time_in, time_out, mod_weight, qkv_weight, out_weight, head_weight,
):
    out = whole(
        timestep, guide_num, guide_den, text_ids, latent,
        text_table, time_in, time_out.T, mod_weight.T, qkv_weight, out_weight, head_weight.T,
    )
    return jnp.swapaxes(out, 1, 2)


def solution(mesh):
    in_specs = (
        P("seq", None, None), P("cfg", None), P(), P(), P(), P("seq", None),
        P(), P(None, "seq"), P(None, "seq"), P(), P(), P(),
    )
    return jax.shard_map(
        on_device, mesh=mesh, in_specs=in_specs, out_specs=P("seq", None, None), check_vma=False
    )
```

```python
import functools
import math

import jax
import jax.numpy as jnp
from jax import lax
from jax.experimental import pallas as pl
from jax.experimental.pallas import tpu as pltpu
from jax.sharding import PartitionSpec as P

HEADS = 24
FREQ = 256
NORM_FLOOR = 0.1
GROUP = 8
PACK = 2
SLICE = 512
VMEM_BYTES = 60 * 1024 * 1024
MESH = pl.DeviceIdType.MESH


def layer_norm(values):
    center = values - jnp.mean(values, axis=-1, keepdims=True)
    spread = jnp.mean(center * center, axis=-1, keepdims=True)
    return center * lax.rsqrt(spread + NORM_FLOOR)


def silu(values):
    return values / (1.0 + jnp.exp(-values))


def each(low, high, act):
    def run(k, carry):
        act(k)
        return carry

    lax.fori_loop(low, high, run, 0)


def many(low, high, act):
    def run(k, carry):
        act(k)
        return carry

    lax.fori_loop(low, high, run, 0, unroll=True)


def whole_kernel(
    n_cfg, n_seq, head_dim, step_hbm, num_hbm, den_hbm, ids_hbm, latent_ref, table_hbm, tin_hbm,
    tout_hbm, mod_w_hbm, wqkv_hbm, wo_hbm, wh_hbm, out_ref,
    step, num, den, ids_ref, table, tin, tout, mod_w, wqkv, wo, wh, lat, slots, mods, mod_all,
    normed, qkv, mixed, branch, finals, spare, preds, landed, load_sem, msg_sem, mod_sem, own_sem,
    lat_sem, ret_send, ret_recv,
):
    cfg, me = lax.axis_index("cfg"), lax.axis_index("seq")
    total = n_cfg * n_seq
    mine = cfg * n_seq + me
    half_seq = n_seq // 2
    side, spot = me // half_seq, lax.rem(me, half_seq)
    edge = jnp.where((2 * me // half_seq == 0) | (2 * me // half_seq == 3), 1, 0)
    frames, pixels, width = latent_ref.shape
    items = pixels // n_cfg // n_seq
    groups, all_frames = lat.shape[0], lat.shape[1]
    rows = all_frames * GROUP
    part_rows, part_frames = rows // 2, all_frames // 2
    tokens = ids_ref.shape[1]
    voc = table.shape[0]
    out_ch = wh.shape[0] // PACK
    pairs = preds.shape[0]
    batch = normed.shape[0] // rows * 2 // n_cfg

    loads = []
    for n, (src, dst) in enumerate(
        (
            (ids_hbm, ids_ref), (step_hbm, step), (tin_hbm, tin), (tout_hbm, tout),
            (mod_w_hbm, mod_w), (num_hbm, num), (den_hbm, den),
            (wqkv_hbm, wqkv), (wo_hbm, wo), (wh_hbm, wh.at[:out_ch]), (wh_hbm, wh.at[out_ch:]),
        )
    ):
        loads.append(pltpu.make_async_copy(src, dst, load_sem.at[n]))
    cuts = list(range(0, voc, SLICE)) + [voc]
    strips = []
    for n, (low, high) in enumerate(zip(cuts[:-1], cuts[1:])):
        strip = slice(low, high)
        strips.append((strip, pltpu.make_async_copy(
            table_hbm.at[strip], table.at[strip], load_sem.at[len(loads) + n]
        )))
    loads[0].start()
    loads[1].start()
    loads[2].start()
    strips[0][1].start()
    loads[3].start()
    for _, strip_copy in strips[1:]:
        strip_copy.start()

    def device(flat):
        return (flat // n_seq, lax.rem(flat, n_seq))

    barrier = pltpu.get_barrier_semaphore()
    each(1, total, lambda k: pl.semaphore_signal(
        barrier, inc=1, device_id=device(lax.rem(mine + k, total)), device_id_type=MESH
    ))

    def piece(owner, g):
        start = pl.multiple_of(cfg * (pixels // n_cfg) + owner * items + g * GROUP, GROUP)
        return latent_ref.at[:, pl.ds(start, GROUP), :]

    def place(source, at_side):
        return lax.rem(source + n_seq - at_side * half_seq, n_seq) * frames

    def near_copy(g, k):
        peer = side * half_seq + lax.rem(spot + k, half_seq)
        return pltpu.make_async_remote_copy(
            src_ref=piece(peer, g), dst_ref=lat.at[g, pl.ds(place(me, side), frames)],
            send_sem=lat_sem.at[2 * groups], recv_sem=lat_sem.at[g],
            device_id=(cfg, peer), device_id_type=MESH,
        )

    def far_copy(g, k):
        peer = (1 - side) * half_seq + lax.rem(spot + k + half_seq // 2, half_seq)
        return pltpu.make_async_remote_copy(
            src_ref=piece(peer, g), dst_ref=lat.at[g, pl.ds(place(me, 1 - side), frames)],
            send_sem=lat_sem.at[2 * groups], recv_sem=lat_sem.at[groups + g],
            device_id=(cfg, peer), device_id_type=MESH,
        )

    def own_copy(g):
        return pltpu.make_async_copy(
            piece(me, g), lat.at[g, pl.ds(place(me, side), frames)], own_sem.at[g]
        )

    def volley(nears, fars, on):
        nears = [g for g in nears if g < groups]
        fars = [g for g in fars if g < groups]

        def shot(k):
            for g in nears:
                near_copy(g, k).start()
            for g in fars:
                far_copy(g, k).start()

        for g in fars:
            send_far(g, 0, on)
        each(1, 1 + (half_seq - 1) * on, shot)

    def send_far(g, low, high):
        each(low, high, lambda k: far_copy(g, k).start())

    def msg_copy(k):
        peer = lax.rem(me + k, n_seq)
        return pltpu.make_async_remote_copy(
            src_ref=slots.at[me], dst_ref=slots.at[me], send_sem=msg_sem.at[0],
            recv_sem=msg_sem.at[1], device_id=(cfg, peer), device_id_type=MESH,
        )

    def mod_copy(k):
        return pltpu.make_async_remote_copy(
            src_ref=mods.at[mine], dst_ref=mods.at[mine], send_sem=mod_sem.at[0],
            recv_sem=mod_sem.at[1], device_id=device(lax.rem(mine + k, total)),
            device_id_type=MESH,
        )

    def ret_copy(q, k):
        flat = lax.rem(mine + k, total)
        return pltpu.make_async_remote_copy(
            src_ref=preds.at[q, pl.ds(place(lax.rem(flat, n_seq), side), frames)],
            dst_ref=landed.at[q, mine], send_sem=ret_send.at[q], recv_sem=ret_recv.at[q],
            device_id=device(flat), device_id_type=MESH,
        )

    def drain(ref, sem):
        pltpu.make_async_copy(ref, ref, sem).wait()
    loads[0].wait()
    ids = jnp.broadcast_to(ids_ref[...] - me * voc, (128, tokens)).T
    lanes = lax.broadcasted_iota(jnp.int32, (tokens, 128), 1)
    tiles = []
    for t in range(-(-voc // 128)):
        hits = jnp.where(ids == lanes + t * 128, 1.0, 0.0)
        tiles.append(jnp.sum(hits, axis=0, keepdims=True))
    counts = jnp.concatenate(tiles, axis=1)[:, :voc]
    high = jnp.floor(counts * (1.0 / 256.0)) * 256.0
    counts = jnp.concatenate([high, counts - high], axis=0).astype(jnp.bfloat16)
    loads[1].wait()
    time = jnp.full((1, FREQ // 2), step[0], jnp.int32).astype(jnp.float32)
    ladder = lax.broadcasted_iota(jnp.int32, (1, FREQ // 2), 1).astype(jnp.float32)
    angles = time * jnp.exp(-math.log(10000.0) * ladder / (FREQ // 2))
    time_freq = jnp.concatenate([jnp.cos(angles), jnp.sin(angles)], axis=1).astype(jnp.bfloat16)
    loads[2].wait()
    hidden = silu(jnp.dot(time_freq, tin[...], preferred_element_type=jnp.float32))
    loads[3].wait()
    time_part = lax.dot_general(
        hidden.astype(jnp.bfloat16), tout[...], (((1,), (1,)), ((), ())),
        preferred_element_type=jnp.float32,
    )
    lane = lax.broadcasted_iota(jnp.int32, (1, width), 1)
    first = me * tout.shape[0]
    placed = jnp.where(
        (lane >= first) & (lane < first + tout.shape[0]),
        jnp.concatenate([time_part] * n_seq, axis=1), 0.0,
    )
    sums = jnp.zeros((2, width), jnp.float32)
    for strip, strip_copy in strips:
        strip_copy.wait()
        sums += jnp.dot(counts[:, strip], table[strip, :], preferred_element_type=jnp.float32)
    for n in range(4, 11):
        loads[n].start()
    pooled = jnp.sum(sums, axis=0, keepdims=True) * (1.0 / math.sqrt(tokens)) + placed
    slots[me] = pooled
    pl.semaphore_wait(barrier, total - 1)
    many(1, n_seq, lambda k: msg_copy(k).start())
    for g in range(groups):
        own_copy(g).start()
    volley([0, 1], [], edge)
    volley([0], [0], 1 - edge)
    volley([1], [], 1 - edge)
    loads[4].wait()
    drain(slots.at[pl.ds(0, n_seq - 1)], msg_sem.at[1])
    cond = silu(jnp.sum(slots[...], axis=0)).astype(jnp.bfloat16)
    mods[mine] = lax.dot_general(
        cond, mod_w[...], (((1,), (1,)), ((), ())), preferred_element_type=jnp.float32
    )
    many(1, total, lambda k: mod_copy(k).start())
    volley([2, 3], [], edge)
    send_far(0, 0, half_seq * edge)
    volley([], [1], edge)
    volley([2, 3], [1], 1 - edge)
    for n in range(5, 11):
        loads[n].wait()
    drain(mods.at[pl.ds(0, total - 1)], mod_sem.at[1])
    for c in range(n_cfg):
        mod_all[c : c + 1] = jnp.concatenate(
            [mods[c * n_seq + s] for s in range(n_seq)], axis=1
        )

    def modulation(c, n):
        return mod_all[c : c + 1, n * width : (n + 1) * width]

    chunk = 4 * head_dim
    steps = width // chunk
    pair = 2 * head_dim
    slab = rows // 4
    slab_frames = all_frames // 4
    lane = lax.broadcasted_iota(jnp.int32, (1, pair), 1)
    left = jnp.where(lane < head_dim, 1.0, 0.0).astype(jnp.bfloat16)
    right = jnp.where(lane < head_dim, 0.0, 1.0).astype(jnp.bfloat16)
    same = lax.broadcasted_iota(jnp.int32, (1, GROUP, rows), 1) == lax.rem(
        lax.broadcasted_iota(jnp.int32, (1, GROUP, rows), 2), GROUP
    )
    shares = jnp.concatenate(
        [jnp.broadcast_to(left, (rows, pair)), jnp.broadcast_to(right, (rows, pair))], axis=0
    )
    top = jnp.full((1, PACK * out_ch), num[0], jnp.int32).astype(jnp.float32)
    bottom = jnp.full((1, PACK * out_ch), den[0], jnp.int32).astype(jnp.float32)
    guide_scale = top / bottom

    def near_arrive(g):
        own_copy(g).wait()
        drain(lat.at[g, pl.ds(0, part_frames - frames)], lat_sem.at[g])

    def far_arrive(g):
        drain(lat.at[g, pl.ds(0, part_frames)], lat_sem.at[groups + g])

    def latent(g, r):
        x = lat[g, r * slab_frames : (r + 1) * slab_frames].astype(jnp.float32)
        return x.reshape(slab, width)

    def prepare(g, r, at):
        n = layer_norm(latent(g, r))
        for c in range(n_cfg):
            y = n * (1.0 + modulation(c, 1)) + modulation(c, 0)
            start = at + c * part_rows + (r % 2) * slab
            normed[start : start + slab, :] = y.astype(jnp.bfloat16)

    def project(owners, first, j):
        x = normed[: len(owners) * n_cfg * part_rows]
        for part in range(3):
            at = slice(part * width + j * chunk, part * width + (j + 1) * chunk)
            out = jnp.dot(x, wqkv[:, at], preferred_element_type=jnp.float32)
            if part == 0:
                out = out * (1.0 / math.sqrt(head_dim))
            out = out.astype(jnp.bfloat16)
            for n, g in enumerate(owners):
                for c in range(n_cfg):
                    start = (n * n_cfg + c) * part_rows
                    qkv[g, c, first : first + part_rows, at] = out[start : start + part_rows]

    def attend(g, c, h):
        kk = qkv[g, c, :, width + h * pair : width + (h + 1) * pair]
        vv = qkv[g, c, :, 2 * width + h * pair : 2 * width + (h + 1) * pair]
        keys = jnp.concatenate([kk * left, kk * right], axis=0)
        vals = jnp.concatenate([vv * left, vv * right], axis=0)
        vals = jnp.concatenate([vals, shares], axis=1)
        scores = lax.dot_general(
            qkv[g, c, :, h * pair : (h + 1) * pair], keys, (((1,), (1,)), ((), ())),
            preferred_element_type=jnp.float32,
        )
        probs = []
        for s in range(2):
            t = scores[:, s * rows : (s + 1) * rows].reshape(all_frames, GROUP, rows)
            t = jnp.where(same, t, -jnp.inf).reshape(rows, rows)
            e = jnp.exp(t - jnp.max(t, axis=1, keepdims=True))
            probs.append(e.astype(jnp.bfloat16))
        both = jnp.dot(
            jnp.concatenate(probs, axis=1), vals, preferred_element_type=jnp.float32
        )
        o = both[:, :pair] / both[:, pair:]
        o = o.astype(jnp.bfloat16)
        for part in range(2):
            start = (part * n_cfg + c) * part_rows
            mixed[start : start + part_rows, h * pair : (h + 1) * pair] = o[
                part * part_rows : (part + 1) * part_rows
            ]

    def leave(part, j):
        at = slice(j * chunk, (j + 1) * chunk)
        block = slice(part * rows, (part + 1) * rows)
        branch[block, at] = jnp.dot(mixed[block, :], wo[:, at], preferred_element_type=jnp.float32)

    def settle(g, r):
        x = latent(g, r)
        for c in range(n_cfg):
            start = (r // 2 * n_cfg + c) * part_rows + r % 2 * slab
            residual = x + modulation(c, 2) * branch[start : start + slab, :]
            final = layer_norm(residual) * (1.0 + modulation(c, 4)) + modulation(c, 3)
            finals[start : start + slab, :] = final.astype(jnp.bfloat16)

    def guide(part):
        block = slice(part * rows, (part + 1) * rows)
        both = lax.dot_general(
            finals[block, :], wh[...], (((1,), (1,)), ((), ())), preferred_element_type=jnp.float32
        )
        guided = both[part_rows:] + guide_scale * (both[:part_rows] - both[part_rows:])
        spare[part * part_frames : (part + 1) * part_frames] = guided.reshape(
            part_frames, GROUP, PACK * out_ch
        ).astype(spare.dtype)

    def finish(g):
        for j in range(steps):
            leave(0, j)
        for j in range(steps):
            leave(1, j)
            if j in (1, 3):
                settle(g, j // 2)
        guide(0)
        settle(g, 2)
        settle(g, 3)
        guide(1)

    def send_pair(q):
        many(1, total, lambda k: ret_copy(q, k).start())
        landed[q, mine] = preds[q, pl.ds(place(me, side), frames)]

    def give(g):
        q = g // PACK

        @pl.when(lax.rem(g, PACK) == 0)
        def _():
            preds[q] = spare[...]

        @pl.when(lax.rem(g, PACK) != 0)
        def _():
            preds[q, :, :, out_ch:] = spare[:, :, out_ch:]

        @pl.when((lax.rem(g, PACK) == 0) & (g > 0))
        def _():
            send_pair(q - 1)

        @pl.when(g == groups - 1)
        def _():
            send_pair(q)

    def attention(g):
        def one(n, carry):
            for c in range(n_cfg):
                for h in range(width // pair):
                    attend(g, c, h)
            return carry

        lax.fori_loop(0, 1, one, 0)

    def near_wave(b, carry):
        owners = [b * batch + n for n in range(batch)]
        for g in owners:
            near_arrive(g)
        for n, g in enumerate(owners):
            for r in range(2):
                prepare(g, r, n * n_cfg * part_rows)
        for j in range(steps):
            project(owners, 0, j)

        @pl.when(2 + b < groups)
        def _():
            send_far(2 + b, 0, half_seq)
        return carry
    lax.fori_loop(0, groups // batch, near_wave, 0)
    for g in range(2 + groups // batch, groups):
        send_far(g, 0, half_seq)

    def far_wave(g, carry):
        far_arrive(g)
        for r in range(2, 4):
            prepare(g, r, 0)
        for j in range(steps):
            project([g], part_rows, j)
        attention(g)
        finish(g)
        give(g)
        return carry

    lax.fori_loop(0, groups, far_wave, 0)
    drain(slots.at[pl.ds(0, n_seq - 1)], msg_sem.at[0])
    drain(mods.at[pl.ds(0, total - 1)], mod_sem.at[0])
    drain(lat.at[:, pl.ds(0, all_frames - frames)], lat_sem.at[2 * groups])
    for q in range(pairs):
        drain(landed.at[q, pl.ds(0, total - 1)], ret_recv.at[q])
        drain(landed.at[q, pl.ds(0, total - 1)], ret_send.at[q])
    per = 128 // GROUP
    for f in range(frames):
        slabs = []
        for source in range(total):
            for g in range(groups):
                tile = landed[g // PACK, source, f].astype(jnp.float32)
                if g % PACK:
                    tile = pltpu.roll(tile, out_ch, 1)
                slabs.append(tile)
        for n in range(pixels // 128):
            block = jnp.concatenate(slabs[n * per : (n + 1) * per], axis=0)
            out_ref[f, :, n * 128 : (n + 1) * 128] = block.T[:out_ch]


def whole(step, num, den, ids, latent, table, tin, tout, mod_w, wqkv, wo, wh):
    n_cfg, n_seq = lax.axis_size("cfg"), lax.axis_size("seq")
    frames, pixels, width = latent.shape
    head_dim = width // HEADS
    items = pixels // n_cfg // n_seq
    groups, all_frames = items // GROUP, frames * n_seq
    rows = all_frames * GROUP
    total = n_cfg * n_seq
    pairs = -(-groups // PACK)
    mod_cols = mod_w.shape[0]
    out_ch = wh.shape[0]
    hbm = pl.BlockSpec(memory_space=pl.ANY)
    bf16 = jnp.bfloat16
    dma = pltpu.SemaphoreType.DMA
    return pl.pallas_call(
        functools.partial(whole_kernel, n_cfg, n_seq, head_dim),
        out_shape=pltpu.VMEM((frames, out_ch, pixels), jnp.float32),
        in_specs=[pl.BlockSpec(memory_space=pltpu.HBM)] * 3 + [hbm] * 9,
        out_specs=pl.BlockSpec(memory_space=pltpu.VMEM),
        scratch_shapes=[
            pltpu.SMEM((1,), jnp.int32),
            pltpu.SMEM((1,), jnp.int32),
            pltpu.SMEM((1,), jnp.int32),
            pltpu.VMEM(ids.shape, jnp.int32),
            pltpu.VMEM(table.shape, bf16),
            pltpu.VMEM(tin.shape, bf16),
            pltpu.VMEM(tout.shape, bf16),
            pltpu.VMEM(mod_w.shape, bf16),
            pltpu.VMEM(wqkv.shape, bf16),
            pltpu.VMEM(wo.shape, bf16),
            pltpu.VMEM((PACK * out_ch, width), bf16),
            pltpu.VMEM((groups, all_frames, GROUP, width), bf16),
            pltpu.VMEM((n_seq, 1, width), jnp.float32),
            pltpu.VMEM((total, 1, mod_cols), jnp.float32),
            pltpu.VMEM((n_cfg, n_seq * mod_cols), jnp.float32),
            pltpu.VMEM((min(2, groups) * n_cfg * rows // 2, width), bf16),
            pltpu.VMEM((groups, n_cfg, rows, 3 * width), bf16),
            pltpu.VMEM((n_cfg * rows, width), bf16),
            pltpu.VMEM((n_cfg * rows, width), jnp.float32),
            pltpu.VMEM((n_cfg * rows, width), bf16),
            pltpu.VMEM((all_frames, GROUP, PACK * out_ch), bf16),
            pltpu.VMEM((pairs, all_frames, GROUP, PACK * out_ch), bf16),
            pltpu.VMEM((pairs, total, frames, GROUP, PACK * out_ch), bf16),
            dma((11 + -(-table.shape[0] // SLICE),)), dma((2,)), dma((2,)), dma((groups,)),
            dma((2 * groups + 1,)), dma((pairs,)), dma((pairs,)),
        ],
        compiler_params=pltpu.CompilerParams(
            collective_id=0, has_side_effects=True, vmem_limit_bytes=VMEM_BYTES
        ),
        name="whole",
    )(step, num, den, ids, latent, table, tin, tout, mod_w, wqkv, wo, wh)


def on_device(
    latent, text_ids, timestep, guide_num, guide_den, text_table,
    time_in, time_out, mod_weight, qkv_weight, out_weight, head_weight,
):
    out = whole(
        timestep, guide_num, guide_den, text_ids, latent,
        text_table, time_in, time_out.T, mod_weight.T, qkv_weight, out_weight, head_weight.T,
    )
    return jnp.swapaxes(out, 1, 2)


def solution(mesh):
    in_specs = (
        P("seq", None, None), P("cfg", None), P(), P(), P(), P("seq", None),
        P(), P(None, "seq"), P(None, "seq"), P(), P(), P(),
    )
    return jax.shard_map(
        on_device, mesh=mesh, in_specs=in_specs, out_specs=P("seq", None, None), check_vma=False
    )
```
